32 devices in a mesh: dp: 16 (over z, y, x), head: 2 (over core).
Axes of the slice: x: 2, y: 2, z: 4, core: 2. Of those that a mesh axis runs over, the one named last changes fastest.
Arguments:
- gradients: float32 [3, 32, 64, 16384], P(None, 'head', None, 'dp'), may hold values from -0.6777015 to 0.6777015
- preconditioner: float32 [3, 32, 64, 64], P(None, 'head'), may hold values from -0.75 to 0.75
- partners: int32 [64, 7], P('dp'), may hold values from -1 to 63, as said below
Outputs:
- tiles: float32 [256, 64, 7, 256], P('head', 'dp')
The draws below stay inside these ranges and needn't reach their ends.
Inputs may be any that keep to these rules, and one draw needn't show every extreme that they name: `partners`: blocks fall into clusters of consecutive blocks, each of at most 8 blocks; row a lists the blocks after a in its cluster in ascending order (slot k holds a + k + 1), then -1 in the remaining slots, so every unordered pair of distinct blocks of a cluster appears once. Some block has all 7 slots filled.
All inputs are finite; a program needn't handle non-finite values.
Results may differ from the reference program's by a relative error of at most 0.013.
Values may be sent and summed in bfloat16 or wider, within the bound.
No kernel may reach another device: no remote copies, remote signals or barrier semaphores. Data moves between devices by JAX's collectives and lax.ppermute only.
A program may use at most 128 MiB of HBM per device.

```python
import jax
import jax.numpy as jnp
from jax import lax

HEADS = 32
HEAD_DIM = 64
LAYERS = 3
BS = 256
BLOCKS_DEV = 4
REACH = 7
N_BLOCKS = 64
EXAMPLES = 16384
N_HEAD = 2


def draw_partners(key, part):
    key_offset, key_extra, key_chosen = jax.random.split(jax.random.fold_in(key, 17), 3)
    cluster_most = REACH + 1
    grid_offset = jax.random.randint(key_offset, (), 1, BLOCKS_DEV)
    position = jnp.arange(N_BLOCKS, dtype=jnp.int32)
    on_grid = (position - grid_offset) % cluster_most == 0
    extra_start = jax.random.randint(key_extra, (N_BLOCKS,), 0, 24) == 0
    choices_left = (N_BLOCKS - grid_offset) // cluster_most
    chosen = grid_offset + cluster_most * jax.random.randint(key_chosen, (), 0, choices_left)
    inside = (position > chosen) & (position < chosen + cluster_most)
    starts = (on_grid | extra_start | (position == 0) | (position == chosen)) & jnp.logical_not(inside)
    cluster = jnp.cumsum(starts.astype(jnp.int32))
    step_ahead = jnp.arange(1, REACH + 1, dtype=jnp.int32)
    target = position[:, None] + step_ahead[None, :]
    clipped = jnp.minimum(target, N_BLOCKS - 1)
    same_cluster = (target < N_BLOCKS) & (cluster[clipped] == cluster[:, None])
    return jnp.where(same_cluster, target, -1).astype(jnp.int32)


def steps_of(own_key, shape, cuts, low, high):
    gain = 1.0
    for dim, blocks in cuts:
        steps = jax.random.uniform(jax.random.fold_in(jax.random.fold_in(own_key, 6), dim), (blocks,), jnp.float32, low / len(cuts), high / len(cuts))
        gain = gain * jnp.repeat(jnp.exp(steps), shape[dim] // blocks).reshape((-1,) + (1,) * (len(shape) - 1 - dim))
    return gain


def centred(rng, dims, scale, most, cuts=(), held_as=jnp.bfloat16):
    loudness = steps_of(rng, dims, cuts, -0.22, 0.18) if cuts else 1.0
    entries = jax.random.normal(rng, dims, jnp.float32) * scale * loudness
    return jnp.minimum(jnp.maximum(entries, -most), most).astype(held_as)


def setup_inputs(seed: int = 0) -> dict:
    streams_of = jax.random.split(jax.random.key(seed), 4)
    return {
        "gradients": centred(streams_of[0], (LAYERS, HEADS, HEAD_DIM, EXAMPLES), ((LAYERS * HEADS * HEAD_DIM) ** -0.25), 0.6777015, ((1, 2), (3, 16)), jnp.float32),
        "preconditioner": centred(streams_of[1], (LAYERS, HEADS, HEAD_DIM, HEAD_DIM), HEAD_DIM ** -0.5, 0.75, ((1, 2),), jnp.float32),
        "partners": draw_partners(jax.random.fold_in(streams_of[3], 71), 0),
    }


def reference(gradients, preconditioner, partners):
    layers, head_count, head_depth, examples = gradients.shape
    blocks = examples // BS
    group_heads = head_count // N_HEAD
    group_rows = layers * group_heads * head_depth
    scaled = jnp.einsum("lhde,lhdn->lhen", preconditioner, gradients, precision=lax.Precision.HIGHEST)

    def grouped(values):
        rounded = values.astype(jnp.bfloat16)
        shaped = rounded.reshape(layers, N_HEAD, group_heads, head_depth, blocks, BS)
        return shaped.transpose(1, 0, 2, 3, 4, 5).reshape(N_HEAD, group_rows, blocks, BS)

    scaled_groups = grouped(scaled)
    plain_groups = grouped(gradients)

    def one_block(block_index):
        own_rows = jnp.take(scaled_groups, block_index, axis=2).astype(jnp.float32)
        partner_ids = partners[block_index]
        clamped = jnp.maximum(partner_ids, 0).astype(jnp.int32)
        partner_cols = jnp.take(plain_groups, clamped, axis=2).astype(jnp.float32)
        partial_value = jnp.einsum("gci,gckj->gikj", own_rows, partner_cols, precision=lax.Precision.HIGHEST)
        live_slot = (partner_ids >= 0).astype(jnp.float32)
        partial_value = (partial_value * live_slot[None, None, :, None]).astype(jnp.bfloat16).astype(jnp.float32)
        return jnp.sum(partial_value, axis=0)

    tiles = lax.map(one_block, jnp.arange(blocks, dtype=jnp.int32))
    return tiles.transpose(1, 0, 2, 3)
```

```python
import functools

import jax
import jax.numpy as jnp
from jax import lax
from jax.experimental import pallas as pl
from jax.experimental.pallas import tpu as pltpu
from jax.sharding import PartitionSpec as P

CHUNKS = 4
ANY = pl.ANY


def cast_kernel(lead, grad_ref, whole_ref, lead_ref):
    low = grad_ref[...].astype(jnp.bfloat16)
    whole_ref[...] = low
    lead_ref[...] = low[:, :lead]


def cast_chunk(rows, chunk, chunk_rows, lead):
    examples = rows.shape[1]
    steps = 3
    tile = chunk_rows // steps
    return pl.pallas_call(
        functools.partial(cast_kernel, lead),
        grid=(steps,),
        in_specs=[pl.BlockSpec((tile, examples), lambda s: (chunk * steps + s, 0))],
        out_specs=[
            pl.BlockSpec((tile, examples), lambda s: (s, 0)),
            pl.BlockSpec((tile, lead), lambda s: (s, 0)),
        ],
        out_shape=[
            jax.ShapeDtypeStruct((chunk_rows, examples), jnp.bfloat16),
            jax.ShapeDtypeStruct((chunk_rows, lead), jnp.bfloat16),
        ],
        name=f"cast_{chunk}",
        cost_estimate=pl.CostEstimate(
            flops=chunk_rows * examples, bytes_accessed=8 * chunk_rows * examples, transcendentals=0
        ),
    )(rows)


def scale_kernel(heads, plain_ref, matrix_ref, out_ref):
    parts = []
    depth = matrix_ref.shape[1]
    for head in range(heads):
        parts.append(
            lax.dot_general(
                matrix_ref[head].astype(jnp.bfloat16),
                plain_ref[head * depth : (head + 1) * depth, :],
                (((0,), (0,)), ((), ())),
                preferred_element_type=jnp.float32,
            )
        )
    out_ref[...] = jnp.concatenate(parts, axis=0).T.astype(jnp.bfloat16)


def scale_chunk(plain, matrices, chunk, block_size):
    chunk_rows, examples = plain.shape
    depth = matrices.shape[1]
    heads = chunk_rows // depth
    return pl.pallas_call(
        functools.partial(scale_kernel, heads),
        grid=(examples // block_size,),
        in_specs=[
            pl.BlockSpec((chunk_rows, block_size), lambda s: (0, s)),
            pl.BlockSpec((heads, depth, depth), lambda s: (chunk, 0, 0)),
        ],
        out_specs=pl.BlockSpec((block_size, chunk_rows), lambda s: (s, 0)),
        out_shape=jax.ShapeDtypeStruct((examples, chunk_rows), jnp.bfloat16),
        name=f"scale_{chunk}",
        cost_estimate=pl.CostEstimate(
            flops=8 * chunk_rows * depth * examples, bytes_accessed=4 * chunk_rows * examples, transcendentals=0
        ),
    )(plain, matrices)


def load_window(count, blocks, extra, size, odd, sources, window, sems):
    def copies(parity):
        made = []
        for c in range(count):
            own, from_even, from_odd, second_even, second_odd = sources[c]
            first = from_odd if parity else from_even
            second = second_odd if parity else second_even
            for b in range(2 * blocks + extra):
                if b < blocks:
                    ref, at = own, b
                elif b < 2 * blocks:
                    ref, at = first, b - blocks
                else:
                    ref, at = second, b - 2 * blocks
                made.append(
                    pltpu.make_async_copy(
                        ref.at[:, pl.ds(at * size, size)], window.at[c, b], sems.at[c, b]
                    )
                )
        return made

    for parity in range(2):

        @pl.when(odd == parity)
        def _():
            made = copies(parity)
            for copy in made:
                copy.start()
            for copy in made:
                copy.wait()


def tile_value(count, member, slot, scaled_refs, window):
    total = None
    for c in range(count):
        term = jnp.dot(
            scaled_refs[c][...], window[c, member + 1 + slot], preferred_element_type=jnp.float32
        )
        total = term if total is None else total + term
    return total


def early_kernel(count, blocks, extra, slots, odd_ref, partner_ref, *refs):
    scaled_refs = refs[:count]
    sources = [refs[count + 5 * c : count + 5 * c + 5] for c in range(count)]
    out_ref, window, sems = refs[count + 5 * count :]
    size = out_ref.shape[-1]
    member = pl.program_id(0)

    @pl.when(member == 0)
    def _():
        load_window(count, blocks, extra, size, odd_ref[0], sources, window, sems)

    for slot in range(slots):

        @pl.when(partner_ref[member, slot] >= 0)
        def _():
            out_ref[0, slot] = tile_value(count, member, slot, scaled_refs, window)


def late_kernel(count, blocks, extra, slots, groups, odd_ref, place_ref, partner_ref, *refs):
    scaled_refs = refs[:count]
    sources = [refs[count + 5 * c : count + 5 * c + 5] for c in range(count)]
    rest = refs[count + 5 * count :]
    early_ref = rest[0]
    out_refs = rest[1 : 1 + groups]
    window, sems, tile = rest[1 + groups :]
    size = early_ref.shape[-1]
    member = pl.program_id(0)
    rows = size // groups

    @pl.when(member == 0)
    def _():
        load_window(count, blocks, extra, size, odd_ref[0], sources, window, sems)

    for slot in range(slots):
        live = partner_ref[member, slot] >= 0

        @pl.when(live)
        def _():
            tile[...] = early_ref[0, slot] + tile_value(count, member, slot, scaled_refs, window)
            for step in range(groups):
                group = lax.rem(place_ref[0] + step, groups)
                at = pl.multiple_of(group * rows, rows)
                out_refs[step][0, slot] = tile[pl.ds(at, rows), :].astype(jnp.bfloat16)

        @pl.when(jnp.logical_not(live))
        def _():
            for step in range(groups):
                out_refs[step][0, slot] = jnp.zeros((rows, size), jnp.bfloat16)


def final_kernel(slots, *refs):
    out_ref = refs[-1]
    for slot in range(slots):
        total = refs[0][0, slot].astype(jnp.float32)
        for ref in refs[1:-1]:
            total = total + ref[0, slot].astype(jnp.float32)
        out_ref[:, 0, slot, :] = total


def products(kind, odd, place, partners, scaled, sources, groups, early=None):
    count = len(scaled)
    blocks, slots = partners.shape
    examples, chunk_rows = scaled[0].shape
    size = examples // blocks
    extra = slots - blocks
    smem = pl.BlockSpec(memory_space=pltpu.SMEM)
    flat = [ref for group in sources for ref in group]
    specs = [pl.BlockSpec((size, chunk_rows), lambda m: (m, 0)) for _ in scaled]
    specs += [pl.BlockSpec(memory_space=ANY) for _ in flat]
    block = pl.BlockSpec((1, slots, size, size), lambda m: (m, 0, 0, 0))
    scratch = [
        pltpu.VMEM((count, 2 * blocks + extra, chunk_rows, size), jnp.bfloat16),
        pltpu.SemaphoreType.DMA((count, 2 * blocks + extra)),
    ]
    cost = pl.CostEstimate(
        flops=2 * count * blocks * slots * size * size * chunk_rows,
        bytes_accessed=4 * blocks * slots * size * size,
        transcendentals=0,
    )
    if kind == "early":
        return pl.pallas_call(
            functools.partial(early_kernel, count, blocks, extra, slots),
            grid=(blocks,),
            in_specs=[smem, smem] + specs,
            out_specs=block,
            out_shape=jax.ShapeDtypeStruct((blocks, slots, size, size), jnp.float32),
            scratch_shapes=scratch,
            name="early_tiles",
            cost_estimate=cost,
        )(odd, partners, *scaled, *flat)
    rows = size // groups
    part = pl.BlockSpec((1, slots, rows, size), lambda m: (m, 0, 0, 0))
    return pl.pallas_call(
        functools.partial(late_kernel, count, blocks, extra, slots, groups),
        grid=(blocks,),
        in_specs=[smem, smem, smem] + specs + [block],
        out_specs=[part] * groups,
        out_shape=[jax.ShapeDtypeStruct((blocks, slots, rows, size), jnp.bfloat16)] * groups,
        scratch_shapes=scratch + [pltpu.VMEM((size, size), jnp.float32)],
        name="late_tiles",
        cost_estimate=cost,
    )(odd, place, partners, *scaled, *flat, early)


def final_sum(parts):
    blocks, slots, rows, size = parts[0].shape
    part = pl.BlockSpec((1, slots, rows, size), lambda m: (m, 0, 0, 0))
    return pl.pallas_call(
        functools.partial(final_kernel, slots),
        grid=(blocks,),
        in_specs=[part] * len(parts),
        out_specs=pl.BlockSpec((rows, 1, slots, size), lambda m: (0, m, 0, 0)),
        out_shape=jax.ShapeDtypeStruct((rows, blocks, slots, size), jnp.float32),
        name="final_sum",
    )(*parts)


def per_device(gradients, preconditioner, partners):
    layers, head_count, depth, examples = gradients.shape
    blocks, slots = partners.shape
    size = examples // blocks
    extra = slots - blocks
    lead = extra * size
    devices = lax.axis_size("dp")
    groups = lax.axis_size("head")
    rows = gradients.reshape(layers * head_count * depth, examples)
    matrices = preconditioner.reshape(layers * head_count, depth, depth)
    chunk_rows = rows.shape[0] // CHUNKS

    odd_to_even = [(d + 1, d) for d in range(0, devices - 1, 2)]
    even_to_odd = [(d, d + 1) for d in range(0, devices - 1, 2)]
    even_back = [(d + 2, d) for d in range(0, devices - 2, 2)]
    odd_back = [(d + 2, d) for d in range(1, devices - 2, 2)]

    def send(array, pairs):
        return lax.ppermute(array, "dp", pairs)

    whole, front = [], []
    for chunk in range(CHUNKS):
        w, f = cast_chunk(rows, chunk, chunk_rows, lead)
        whole.append(w)
        front.append(f)

    first_even = [None] * CHUNKS
    first_odd = [None] * CHUNKS
    second_even = [None] * CHUNKS
    second_odd = [None] * CHUNKS
    crossed = send(whole[0], even_to_odd)
    first_even[0] = send(whole[0], odd_to_even)
    for chunk in range(1, CHUNKS):
        second_even[chunk] = send(whole[chunk], even_back)
        second_odd[chunk] = send(front[chunk], odd_back)
        first_even[chunk] = send(whole[chunk], odd_to_even)
    first_odd[0] = send(crossed, odd_back)
    for chunk in range(1, CHUNKS):
        first_odd[chunk] = send(second_even[chunk], even_to_odd)
    second_even[0] = second_odd[0] = send(front[0], even_back + odd_back)

    scaled = [scale_chunk(whole[c], matrices, c, size) for c in range(CHUNKS)]
    odd = lax.rem(lax.axis_index("dp"), 2).reshape(1).astype(jnp.int32)
    place = lax.axis_index("head").reshape(1).astype(jnp.int32)
    sources = [
        [whole[c], first_even[c], first_odd[c], second_even[c], second_odd[c]] for c in range(CHUNKS)
    ]
    early = products("early", odd, place, partners, scaled[:-1], sources[:-1], groups)
    parts = products("late", odd, place, partners, scaled[-1:], sources[-1:], groups, early)
    got = [parts[0]]
    for step in range(1, groups):
        pairs = [(g, (g + step) % groups) for g in range(groups)]
        got.append(lax.ppermute(parts[step], "head", pairs))
    return final_sum(got)


def solution(mesh):
    in_specs = (P(None, "head", None, "dp"), P(None, "head", None, None), P("dp", None))
    out_specs = P("head", "dp", None, None)
    return jax.shard_map(
        per_device, mesh=mesh, in_specs=in_specs, out_specs=out_specs, check_vma=False
    )
```

```python
import functools

import jax
import jax.numpy as jnp
from jax import lax
from jax.experimental import pallas as pl
from jax.experimental.pallas import tpu as pltpu
from jax.sharding import PartitionSpec as P


CHUNKS = 4
ANY = pl.ANY
SPARE = 2 * 1024 * 1024


def cast_kernel(lead, grad_ref, whole_ref, lead_ref):
    low = grad_ref[...].astype(jnp.bfloat16)
    whole_ref[...] = low
    lead_ref[...] = low[:, :lead]


def cast_chunk(rows, chunk, chunk_rows, lead):
    examples = rows.shape[1]
    steps = 3
    tile = chunk_rows // steps
    return pl.pallas_call(
        functools.partial(cast_kernel, lead),
        grid=(steps,),
        in_specs=[pl.BlockSpec((tile, examples), lambda s: (chunk * steps + s, 0))],
        out_specs=[
            pl.BlockSpec((tile, examples), lambda s: (s, 0)),
            pl.BlockSpec((tile, lead), lambda s: (s, 0)),
        ],
        out_shape=[
            jax.ShapeDtypeStruct((chunk_rows, examples), jnp.bfloat16),
            jax.ShapeDtypeStruct((chunk_rows, lead), jnp.bfloat16),
        ],
        compiler_params=pltpu.CompilerParams(vmem_limit_bytes=5 * SPARE),
        cost_estimate=pl.CostEstimate(
            flops=chunk_rows * examples, bytes_accessed=8 * chunk_rows * examples, transcendentals=0
        ),
    )(rows)


def scale_kernel(heads, plain_ref, matrix_ref, out_ref):
    parts = []
    depth = matrix_ref.shape[1]
    for head in range(heads):
        parts.append(
            lax.dot_general(
                matrix_ref[head].astype(jnp.bfloat16),
                plain_ref[head * depth : (head + 1) * depth, :],
                (((0,), (0,)), ((), ())),
                preferred_element_type=jnp.float32,
            )
        )
    out_ref[...] = jnp.concatenate(parts, axis=0).T.astype(jnp.bfloat16)


def scale_chunk(plain, matrices, chunk, block_size):
    chunk_rows, examples = plain.shape
    depth = matrices.shape[1]
    heads = chunk_rows // depth
    return pl.pallas_call(
        functools.partial(scale_kernel, heads),
        grid=(examples // block_size,),
        in_specs=[
            pl.BlockSpec((chunk_rows, block_size), lambda s: (0, s)),
            pl.BlockSpec((heads, depth, depth), lambda s: (chunk, 0, 0)),
        ],
        out_specs=pl.BlockSpec((block_size, chunk_rows), lambda s: (s, 0)),
        out_shape=jax.ShapeDtypeStruct((examples, chunk_rows), jnp.bfloat16),
        compiler_params=pltpu.CompilerParams(vmem_limit_bytes=5 * SPARE),
        cost_estimate=pl.CostEstimate(
            flops=8 * chunk_rows * depth * examples, bytes_accessed=4 * chunk_rows * examples, transcendentals=0
        ),
    )(plain, matrices)


def load_window(spans, blocks, size, odd, sources, window, sems):
    def copies(parity):
        made = []
        at = 0
        for (low, high), (own, from_even, from_odd, second_even, second_odd) in zip(spans, sources):
            first = from_odd if parity else from_even
            second = second_odd if parity else second_even
            for b in range(low, high):
                if b < blocks:
                    ref, column = own, b
                elif b < 2 * blocks:
                    ref, column = first, b - blocks
                else:
                    ref, column = second, b - 2 * blocks
                made.append(
                    pltpu.make_async_copy(
                        ref.at[:, pl.ds(column * size, size)], window.at[at], sems.at[at]
                    )
                )
                at += 1
        return made

    for parity in range(2):

        @pl.when(odd == parity)
        def _():
            made = copies(parity)
            for copy in made:
                copy.start()
            for copy in made:
                copy.wait()


def add_tiles(spans, member, slot, scaled_refs, window, tile, fresh):
    block = member + 1 + slot
    at = 0
    for c, (low, high) in enumerate(spans):
        base = at - low

        def add(c=c, base=base, first=fresh and c == 0):
            term = jnp.dot(
                scaled_refs[c][...], window[base + block], preferred_element_type=jnp.float32
            )
            tile[...] = term if first else tile[...] + term

        if (low, high) == spans[0]:
            add()
        else:
            pl.when(jnp.logical_and(block >= low, block < high))(add)
        at += high - low


def early_kernel(spans, blocks, slots, odd_ref, partner_ref, *refs):
    count = len(spans)
    scaled_refs = refs[:count]
    sources = [refs[count + 5 * c : count + 5 * c + 5] for c in range(count)]
    out_ref, window, sems = refs[6 * count :]
    member = pl.program_id(0)

    @pl.when(member == 0)
    def _():
        load_window(spans, blocks, out_ref.shape[-1], odd_ref[0], sources, window, sems)

    for slot in range(slots):

        @pl.when(partner_ref[member, slot] >= 0)
        def _():
            add_tiles(spans, member, slot, scaled_refs, window, out_ref.at[0, slot], True)


def late_kernel(spans, blocks, slots, groups, odd_ref, place_ref, partner_ref, *refs):
    count = len(spans)
    scaled_refs = refs[:count]
    sources = [refs[count + 5 * c : count + 5 * c + 5] for c in range(count)]
    rest = refs[6 * count :]
    early_ref = rest[0]
    out_refs = rest[1 : 1 + groups]
    window, sems, tile = rest[1 + groups :]
    size = early_ref.shape[-1]
    member = pl.program_id(0)
    rows = size // groups

    @pl.when(member == 0)
    def _():
        load_window(spans, blocks, size, odd_ref[0], sources, window, sems)

    for slot in range(slots):
        live = partner_ref[member, slot] >= 0

        @pl.when(live)
        def _():
            tile[...] = early_ref[0, slot]
            add_tiles(spans, member, slot, scaled_refs, window, tile, False)
            for step in range(groups):
                group = lax.rem(place_ref[0] + step, groups)
                at = pl.multiple_of(group * rows, rows)
                out_refs[step][0, slot] = tile[pl.ds(at, rows), :].astype(jnp.bfloat16)

        @pl.when(jnp.logical_not(live))
        def _():
            for step in range(groups):
                out_refs[step][0, slot] = jnp.zeros((rows, size), jnp.bfloat16)


def final_kernel(blocks, *refs):
    out_ref = refs[-1]
    for block in range(blocks):
        total = refs[0][block, 0].astype(jnp.float32)
        for ref in refs[1:-1]:
            total = total + ref[block, 0].astype(jnp.float32)
        out_ref[:, 0, block, :] = total


def products(spans, odd, place, partners, scaled, sources, groups, early=None):
    blocks, slots = partners.shape
    examples, chunk_rows = scaled[0].shape
    size = examples // blocks
    smem = pl.BlockSpec(memory_space=pltpu.SMEM)
    flat = [ref for group in sources for ref in group]
    specs = [pl.BlockSpec((size, chunk_rows), lambda m: (m, 0)) for _ in scaled]
    specs += [pl.BlockSpec(memory_space=ANY) for _ in flat]
    block = pl.BlockSpec((1, slots, size, size), lambda m: (m, 0, 0, 0))
    held = sum(high - low for low, high in spans)
    scratch = [
        pltpu.VMEM((held, chunk_rows, size), jnp.bfloat16),
        pltpu.SemaphoreType.DMA((held,)),
    ]
    limit = 2 * held * chunk_rows * size + 8 * slots * size * size + 4 * len(spans) * size * chunk_rows
    cost = pl.CostEstimate(
        flops=2 * len(spans) * blocks * slots * size * size * chunk_rows,
        bytes_accessed=4 * blocks * slots * size * size,
        transcendentals=0,
    )
    if early is None:
        return pl.pallas_call(
            functools.partial(early_kernel, spans, blocks, slots),
            grid=(blocks,),
            in_specs=[smem, smem] + specs,
            out_specs=block,
            out_shape=jax.ShapeDtypeStruct((blocks, slots, size, size), jnp.float32),
            scratch_shapes=scratch,
            name="early_tiles",
            compiler_params=pltpu.CompilerParams(vmem_limit_bytes=limit + 2 * SPARE),
            cost_estimate=cost,
        )(odd, partners, *scaled, *flat)
    rows = size // groups
    part = pl.BlockSpec((1, slots, rows, size), lambda m: (m, 0, 0, 0))
    return pl.pallas_call(
        functools.partial(late_kernel, spans, blocks, slots, groups),
        grid=(blocks,),
        in_specs=[smem, smem, smem] + specs + [block],
        out_specs=[part] * groups,
        out_shape=[jax.ShapeDtypeStruct((blocks, slots, rows, size), jnp.bfloat16)] * groups,
        scratch_shapes=scratch + [pltpu.VMEM((size, size), jnp.float32)],
        name="late_tiles",
        compiler_params=pltpu.CompilerParams(vmem_limit_bytes=limit + 4 * slots * size * size + 2 * SPARE),
        cost_estimate=cost,
    )(odd, place, partners, *scaled, *flat, early)


def final_sum(parts):
    blocks, slots, rows, size = parts[0].shape
    part = pl.BlockSpec((blocks, 1, rows, size), lambda s: (0, s, 0, 0))
    tiles = pl.pallas_call(
        functools.partial(final_kernel, blocks),
        grid=(slots,),
        in_specs=[part] * len(parts),
        out_specs=pl.BlockSpec((rows, 1, blocks, size), lambda s: (0, s, 0, 0)),
        out_shape=jax.ShapeDtypeStruct((rows, slots, blocks, size), jnp.float32),
        name="final_sum",
        compiler_params=pltpu.CompilerParams(vmem_limit_bytes=4 * SPARE),
    )(*parts)
    return tiles.transpose(0, 2, 1, 3)


def per_device(gradients, preconditioner, partners):
    layers, head_count, depth, examples = gradients.shape
    blocks, slots = partners.shape
    size = examples // blocks
    extra = slots - blocks
    lead = extra * size
    devices = lax.axis_size("dp")
    groups = lax.axis_size("head")
    rows = gradients.reshape(layers * head_count * depth, examples)
    matrices = preconditioner.reshape(layers * head_count, depth, depth)
    chunk_rows = rows.shape[0] // CHUNKS

    odd_to_even = [(d + 1, d) for d in range(0, devices - 1, 2)]
    even_to_odd = [(d, d + 1) for d in range(0, devices - 1, 2)]
    even_back = [(d + 2, d) for d in range(0, devices - 2, 2)]
    odd_back = [(d + 2, d) for d in range(1, devices - 2, 2)]

    def send(array, pairs):
        return lax.ppermute(array, "dp", pairs)

    whole, front = [], []
    for chunk in range(CHUNKS):
        w, f = cast_chunk(rows, chunk, chunk_rows, lead)
        whole.append(w)
        front.append(f)

    first_even = [send(whole[c], odd_to_even) for c in range(CHUNKS)]
    crossed = send(whole[0], even_to_odd)
    second_even, second_odd = [None], [None]
    for c in range(1, CHUNKS):
        second_even.append(send(whole[c], even_back))
        second_odd.append(send(front[c], odd_back))
    first_odd = [send(crossed, odd_back)]
    for c in range(1, CHUNKS):
        first_odd.append(send(second_even[c], even_to_odd))
    second_even[0] = second_odd[0] = send(front[0], even_back + odd_back)

    scaled = []
    for c in range(CHUNKS):
        scaled.append(scale_chunk(whole[c], matrices, c, size))
    odd = lax.rem(lax.axis_index("dp"), 2).reshape(1).astype(jnp.int32)
    place = lax.axis_index("head").reshape(1).astype(jnp.int32)
    sources = [
        [whole[c], first_even[c], first_odd[c], second_even[c], second_odd[c]] for c in range(CHUNKS)
    ]
    every = (0, blocks + slots)
    order = list(range(1, CHUNKS - 1)) + [0]
    early = products(
        [every] * (CHUNKS - 2) + [(0, 2 * blocks)],
        odd,
        place,
        partners,
        [scaled[c] for c in order],
        [sources[c] for c in order],
        groups,
    )
    order = [CHUNKS - 1, 0]
    parts = products(
        [every, (2 * blocks, blocks + slots)],
        odd,
        place,
        partners,
        [scaled[c] for c in order],
        [sources[c] for c in order],
        groups,
        early,
    )
    got = [parts[0]]
    for step in range(1, groups):
        pairs = [(g, (g + step) % groups) for g in range(groups)]
        got.append(lax.ppermute(parts[step], "head", pairs))
    return final_sum(got)


def solution(mesh):
    in_specs = (P(None, "head", None, "dp"), P(None, "head", None, None), P("dp", None))
    out_specs = P("head", "dp", None, None)

    return jax.shard_map(
        per_device, mesh=mesh, in_specs=in_specs, out_specs=out_specs, check_vma=False
    )
```
